32 devices in a mesh: edp: 2 (over x), ep: 16 (over z, y, core).
Axes of the slice: x: 2, y: 2, z: 4, core: 2. Of those that a mesh axis runs over, the one named last changes fastest.
Arguments:
- tokens: bfloat16 [4096, 3584], P(('edp', 'ep')), may hold values from -6 to 6
- node_ids: int32 [4096, 4], P(('edp', 'ep')), may hold values from 0 to 7, as said below
- local_ids: int32 [4096, 8], P(('edp', 'ep')), may hold values from 0 to 3, as said below
- affinity: float32 [4096, 8], P(('edp', 'ep')), may hold values from 0.2 to 1
- w_gate: bfloat16 [32, 3584, 1024], P(('edp', 'ep')), may hold values from -0.09375 to 0.09375
- w_up: bfloat16 [32, 3584, 1024], P(('edp', 'ep')), may hold values from -0.09375 to 0.09375
- w_down: bfloat16 [32, 1024, 3584], P(('edp', 'ep')), may hold values from -0.1875 to 0.1875
- grad_parts: float32 [32, 3584, 32], P(('edp', 'ep')), may hold values from -0.6 to 0.6
Outputs:
- mixed: bfloat16 [4096, 3584], P(('edp', 'ep'))
- router_grad: float32 [3584, 32], P(('edp', 'ep'))
The draws below stay inside these ranges and needn't reach their ends.
Inputs may be any that keep to these rules, and one draw needn't show every extreme that they name: `node_ids`: A token's 4 nodes are distinct and increasing. `local_ids`: columns 2 j and 2 j + 1 name the two experts 2 m and 2 m + 1 of one pair m of node node_ids[t, j], in either order. From the 128 tokens of one device each expert receives at most 40 routes; inside a node the loads from one device differ by at most one.
All inputs are finite; a program needn't handle non-finite values.
Results may differ from the reference program's by a relative error of at most 0.0057.
Values may be sent and summed in bfloat16 or wider, within the bound.
A program may use at most 192 MiB of HBM per device.

```python
import math
import jax
import jax.numpy as jnp
from jax import lax

D = 3584
H = 1024
TOK_DEV = 128
TOP = 8
NODE_PICK = 4
GROUPS = 8
EXPERTS = 32
CAP = 40
TOKENS = 4096
N_EDP = 2
N_EP = 16


def routing_plan(key):
    base_key = jax.random.fold_in(key, 7)
    per_node = EXPERTS // GROUPS
    pair_count = per_node // 2
    pairing = jax.random.permutation(jax.random.fold_in(base_key, 1), GROUPS).astype(jnp.int32)

    def block_plan(block):
        block_key = jax.random.fold_in(base_key, block + 100)
        shifts = jax.random.randint(jax.random.fold_in(block_key, 1), (GROUPS // 2,), 0, TOK_DEV // 8 + 1).astype(jnp.int32)
        shifts = shifts.at[0].set(TOK_DEV // 8)
        counts = jnp.zeros((GROUPS,), jnp.int32)
        counts = counts.at[pairing[0::2]].set(TOK_DEV // 2 + shifts)
        counts = counts.at[pairing[1::2]].set(TOK_DEV // 2 - shifts)
        node_major = jnp.repeat(jnp.arange(GROUPS, dtype=jnp.int32), counts, total_repeat_length=NODE_PICK * TOK_DEV)
        chosen = node_major.reshape(NODE_PICK, TOK_DEV).T
        shuffle = jax.random.permutation(jax.random.fold_in(block_key, 2), TOK_DEV)
        chosen = chosen[shuffle]
        onehot = jnp.sum((chosen[:, :, None] == jnp.arange(GROUPS, dtype=jnp.int32)[None, None, :]).astype(jnp.int32), axis=1)
        earlier = jnp.cumsum(onehot, axis=0) - onehot
        ranks = jnp.take_along_axis(earlier, chosen, axis=1)
        offsets = jax.random.randint(jax.random.fold_in(block_key, 3), (GROUPS,), 0, pair_count).astype(jnp.int32)
        pair_index = (ranks + offsets[chosen]) % pair_count
        flips = jax.random.randint(jax.random.fold_in(block_key, 4), (TOK_DEV, NODE_PICK), 0, 2).astype(jnp.int32)
        first = 2 * pair_index + flips
        second = 2 * pair_index + 1 - flips
        local = jnp.stack([first, second], axis=2).reshape(TOK_DEV, TOP)
        return (chosen, local)
    nodes, locals_all = jax.vmap(block_plan)(jnp.arange(EXPERTS, dtype=jnp.int32))
    return (nodes.reshape(-1, NODE_PICK).astype(jnp.int32), locals_all.reshape(-1, TOP).astype(jnp.int32))


def draw_node_ids(key, part):
    return routing_plan(key)[0]


def draw_local_ids(key, part):
    return routing_plan(key)[1]


def with_spikes(entries, rng, source, target, blocks, factor):
    def block_of(position):
        return (jnp.arange(entries.shape[position]) // (entries.shape[position] // blocks)).reshape((-1,) + (1,) * (entries.ndim - 1 - position))

    near = jax.random.permutation(rng, blocks)[block_of(target)]
    far = (block_of(target) + blocks // 2) % blocks
    return jnp.where((block_of(source) == near) | (block_of(source) == far), factor * entries, entries)


def level_of(stream_key, dims, split, least, high):
    factor_of, own = 1.0, jax.random.fold_in(stream_key, 6)
    for axis_at, shards_of in split:
        steps = jnp.exp(jax.random.uniform(jax.random.fold_in(own, axis_at), (shards_of,), jnp.float32, least / len(split), high / len(split)))
        factor_of = factor_of * jnp.repeat(steps, dims[axis_at] // shards_of).reshape([-1 if axis == axis_at else 1 for axis in range(len(dims))])
    return factor_of


def bell_draw(stream_key, shape, spread, most, split=(), held_as=jnp.bfloat16):
    level = level_of(stream_key, shape, split, -0.22, 0.18) if split else 1.0
    values = jax.random.normal(stream_key, shape, jnp.float32) * spread * level
    return jnp.minimum(jnp.maximum(values, -most), most).astype(held_as)


def bell_draw_with(stream_key, dims, scale, limit, shards, heavy, kind=jnp.bfloat16):
    entries = scale * jax.random.normal(stream_key, dims, jnp.float32)
    if shards:
        entries = entries * level_of(stream_key, dims, shards, -0.22, 0.18)
    return jnp.clip(with_spikes(entries, jax.random.fold_in(stream_key, 3), *heavy), -limit, limit).astype(kind)


def setup_inputs(seed: int = 0) -> dict:
    keys = jax.random.split(jax.random.key(seed), 9)
    tokens = bell_draw(keys[0], (TOKENS, D), 1.0, 6.0, ((0, 32),))
    node_ids = draw_node_ids(jax.random.fold_in(keys[8], 71), 0)
    local_ids = draw_local_ids(jax.random.fold_in(keys[8], 71), 0)
    affinity = jnp.clip(jnp.exp(math.log(1.0) - 1.609438 * jax.random.uniform(keys[3], (TOKENS, TOP), jnp.float32) ** level_of(keys[3], (TOKENS, TOP), ((0, 32),), -0.2, 0.2)), 0.2, 1.0)
    w_gate = bell_draw(keys[4], (EXPERTS, D, H), D ** -0.5, 0.09375, ((0, 32),))
    w_up = bell_draw(keys[5], (EXPERTS, D, H), D ** -0.5, 0.09375, ((0, 32),))
    w_down = bell_draw(keys[6], (EXPERTS, H, D), H ** -0.5, 0.1875, ((0, 32),))
    grad_parts = bell_draw_with(keys[7], (N_EDP * N_EP, D, EXPERTS), 0.1, 0.6, ((0, 32),), (0, 1, 32, 2.75), jnp.float32)
    return {"tokens": tokens, "node_ids": node_ids, "local_ids": local_ids, "affinity": affinity, "w_gate": w_gate, "w_up": w_up, "w_down": w_down, "grad_parts": grad_parts}


def reference(tokens, node_ids, local_ids, affinity, w_gate, w_up, w_down, grad_parts):
    per_node = EXPERTS // GROUPS
    expert = (jnp.repeat(node_ids, 2, axis=1) * per_node + local_ids).astype(jnp.int32)
    weight = 2.5 * affinity / jnp.sum(affinity, axis=1, keepdims=True)
    flat_expert = expert.reshape(-1)
    route_order = jnp.argsort(flat_expert, stable=True).astype(jnp.int32)
    counts = jnp.bincount(flat_expert, length=EXPERTS).astype(jnp.int32)
    starts = (jnp.cumsum(counts) - counts).astype(jnp.int32)
    rows_most = CAP * N_EDP * N_EP
    padded_order = jnp.concatenate([route_order, jnp.zeros((rows_most,), jnp.int32)])
    flat_weight = weight.reshape(-1)

    def per_expert(accum, inputs):
        gate_w, up_w, down_w, start, count = inputs
        row_index = lax.dynamic_slice(padded_order, (start.astype(jnp.int32),), (rows_most,))
        is_valid = jnp.arange(rows_most, dtype=jnp.int32) < count
        token_index = row_index // TOP
        row_block = tokens[token_index]
        gate_act = jnp.dot(row_block, gate_w, preferred_element_type=jnp.float32)
        up_act = jnp.dot(row_block, up_w, preferred_element_type=jnp.float32)
        hidden = (jax.nn.silu(gate_act) * up_act).astype(jnp.bfloat16)
        result = jnp.dot(hidden, down_w, preferred_element_type=jnp.float32).astype(jnp.bfloat16)
        scaled = jnp.where(is_valid, flat_weight[row_index], jnp.zeros((), jnp.float32))
        accum = accum.at[token_index].add(scaled[:, None] * result.astype(jnp.float32))
        return accum, None

    start_sum = jnp.zeros(tokens.shape, jnp.float32)
    mixed_sum, _ = lax.scan(per_expert, start_sum, (w_gate, w_up, w_down, starts, counts))
    router_grad = jnp.sum(grad_parts, axis=0)
    return mixed_sum.astype(jnp.bfloat16), router_grad
```

```python
import jax
import jax.numpy as jnp
from jax import lax
from jax.sharding import PartitionSpec as P

GROUPS = 8
AXES = ("edp", "ep")


def body(tokens, node_ids, local_ids, affinity, w_gate, w_up, w_down, grad_parts):
    edp_count = lax.axis_size("edp")
    ep_count = lax.axis_size("ep")
    experts = edp_count * ep_count
    tok_rows, model_width = tokens.shape
    top_routes = local_ids.shape[1]
    node_pick = node_ids.shape[1]
    capacity = 10 * tok_rows // experts
    per_node = experts // GROUPS
    line = ep_count // per_node
    pairs = per_node // 2
    plane = edp_count * pairs
    f32, bf16 = jnp.float32, jnp.bfloat16

    edp_me, ep_me = lax.axis_index("edp"), lax.axis_index("ep")
    node_me = ep_me // per_node
    pair_me = (ep_me % per_node) // 2
    core_me = ep_me % 2
    me = edp_me * ep_count + ep_me
    plane_me = edp_me * pairs + pair_me

    def split(device):
        edp, ep = divmod(device, ep_count)
        node, inner = divmod(ep, per_node)
        pair, core = divmod(inner, 2)
        return edp, node, pair, core

    def join(edp, node, pair, core):
        return edp * ep_count + node * per_node + pair * 2 + core

    def along_line(value, step):
        perm = []
        for device in range(experts):
            edp, node, pair, core = split(device)
            perm.append((device, join(edp, node ^ step, pair, core)))
        return lax.ppermute(value, AXES, perm)

    def in_plane(value, step):
        perm = []
        for device in range(experts):
            edp, node, pair, core = split(device)
            other_edp, other_pair = divmod((edp * pairs + pair) ^ step, pairs)
            perm.append((device, join(other_edp, node, other_pair, core)))
        return lax.ppermute(value, AXES, perm)

    def core_swap(value):
        return lax.ppermute(value, AXES, [(device, device ^ 1) for device in range(experts)])

    grad_rows, grad_cols = grad_parts.shape[1:]
    grad_flat = grad_parts[0].reshape(experts, grad_rows * grad_cols // experts)
    router_grad = lax.psum_scatter(grad_flat, AXES, scatter_dimension=0, tiled=True)
    router_grad = router_grad.reshape(grad_rows // experts, grad_cols)

    expert = jnp.repeat(node_ids, top_routes // node_pick, axis=1) * per_node + local_ids
    weight = 2.5 * affinity / jnp.sum(affinity, axis=1, keepdims=True)
    every = jnp.arange(experts, dtype=jnp.int32)
    dense = jnp.sum(
        jnp.where(expert[:, :, None] == every[None, None, :], weight[:, :, None], 0.0), axis=1
    )
    high = lax.reduce_precision(dense, 8, 7)
    low = dense - high
    spare = -(2 * experts) % 128
    extended = jnp.concatenate(
        [tokens, high.astype(bf16), low.astype(bf16), jnp.zeros((tok_rows, spare), bf16)], axis=1
    )

    rows_iota = jnp.arange(tok_rows, dtype=jnp.int32)
    earlier = (rows_iota[None, :] < rows_iota[:, None]).astype(bf16)
    plane_ids = plane_me ^ jnp.arange(plane, dtype=jnp.int32)
    first_expert = (
        (plane_ids // pairs) * ep_count + node_me * per_node + (plane_ids % pairs) * 2
    )
    pick = (every[:, None] == first_expert[None, :]).astype(bf16)
    slot_ids = jnp.arange(capacity, dtype=jnp.int32)
    mine = jnp.arange(experts, dtype=jnp.int32) == me

    def dispatch(block):
        routed = (block[:, model_width : model_width + experts] != 0).astype(bf16)
        mask = jnp.dot(routed, pick, preferred_element_type=f32)
        slot = jnp.dot(earlier, mask.astype(bf16), preferred_element_type=f32).astype(jnp.int32)
        chosen = (slot.T[:, None, :] == slot_ids[None, :, None]) & (mask.T[:, None, :] > 0)
        select = chosen.astype(bf16).reshape(plane * capacity, tok_rows)
        picked = jnp.dot(select, block, preferred_element_type=f32).astype(bf16)
        picked = picked.reshape(plane, capacity, -1)
        got = [picked[0]] + [in_plane(picked[step], step) for step in range(1, plane)]
        own_rows = jnp.concatenate(got, axis=0)
        return select, own_rows, core_swap(own_rows)

    def expert_rows(own_rows, other_rows):
        rows = jnp.concatenate([own_rows, other_rows], axis=0)
        half = own_rows.shape[0]
        feats = rows[:, :model_width]
        gate_act = jnp.dot(feats, w_gate[0], preferred_element_type=f32)
        up_act = jnp.dot(feats, w_up[0], preferred_element_type=f32)
        hidden = (jax.nn.silu(gate_act) * up_act).astype(bf16)
        result = jnp.dot(hidden, w_down[0], preferred_element_type=f32)
        both = rows[:, model_width : model_width + experts].astype(f32)
        both = both + rows[:, model_width + experts : model_width + 2 * experts].astype(f32)
        scale = jnp.sum(jnp.where(mine[None, :], both, 0.0), axis=1, keepdims=True)
        scaled = (result * scale).astype(bf16)
        other = core_swap(scaled[half:])
        return (scaled[:half].astype(f32) + other.astype(f32)).astype(bf16)

    def combine(select, summed):
        summed = summed.reshape(plane, capacity, model_width)
        back = [summed[0]] + [in_plane(summed[step], step) for step in range(1, plane)]
        back = jnp.concatenate(back, axis=0)
        return lax.dot_general(
            select, back, (((0,), (0,)), ((), ())), preferred_element_type=f32
        )

    blocks = [extended] + [along_line(extended, step) for step in range(1, line)]
    mixed = jnp.zeros((tok_rows, model_width), f32)
    sent = [dispatch(block) for block in blocks]
    for step in range(line):
        select, own_rows, other_rows = sent[step]
        part = combine(select, expert_rows(own_rows, other_rows))
        if step:
            part = along_line(part.astype(bf16), step).astype(f32)
        mixed = mixed + part
    return (mixed.astype(bf16), router_grad)


def solution(mesh):
    placed = (
        P(("edp", "ep"), None),
        P(("edp", "ep"), None),
        P(("edp", "ep"), None),
        P(("edp", "ep"), None),
        P(("edp", "ep"), None, None),
        P(("edp", "ep"), None, None),
        P(("edp", "ep"), None, None),
        P(("edp", "ep"), None, None),
    )
    return jax.shard_map(
        body,
        mesh=mesh,
        in_specs=placed,
        out_specs=(P(("edp", "ep"), None), P(("edp", "ep"), None)),
        check_vma=False,
    )
```

```python
import jax
import jax.numpy as jnp
from jax import lax
from jax.experimental import pallas as pl
from jax.experimental.pallas import tpu as pltpu
from jax.sharding import PartitionSpec as P


GROUPS = 8
AXES = ("edp", "ep")


def select_kernel(block_ref, pick_ref, earlier_ref, spread_ref, slot_ref, select_ref, picked_ref):
    f32 = jnp.float32
    experts = pick_ref.shape[1]
    width = block_ref.shape[1]
    model_width = width - 2 * experts - (-(2 * experts) % 128)
    tail = block_ref[:, model_width:].astype(f32)[:, :experts]
    routed = jnp.where(tail != 0, 1.0, 0.0).astype(f32)
    mask = lax.dot_general(
        pick_ref[...], routed, (((1,), (1,)), ((), ())), preferred_element_type=f32
    )
    slot = jnp.dot(mask, earlier_ref[...], preferred_element_type=f32)
    slot = jnp.dot(spread_ref[...], slot, preferred_element_type=f32)
    mask = jnp.dot(spread_ref[...], mask, preferred_element_type=f32)
    chosen = jnp.where((slot == slot_ref[...]) & (mask > 0.5), 1.0, 0.0).astype(jnp.bfloat16)
    select_ref[...] = chosen
    picked = jnp.dot(chosen, block_ref[...], preferred_element_type=f32)
    picked_ref[...] = picked.astype(jnp.bfloat16)


def select_rows(block, pick, earlier, spread, slot_of):
    rows, tok_rows = slot_of.shape
    width = block.shape[1]
    return pl.pallas_call(
        select_kernel,
        out_shape=(
            jax.ShapeDtypeStruct((rows, tok_rows), jnp.bfloat16),
            jax.ShapeDtypeStruct((rows, width), jnp.bfloat16),
        ),
        compiler_params=pltpu.CompilerParams(vmem_limit_bytes=24 * 1024 * 1024),
        cost_estimate=pl.CostEstimate(
            flops=2 * rows * tok_rows * width, bytes_accessed=6 * rows * width, transcendentals=0
        ),
    )(block, pick, earlier, spread, slot_of)


def join_kernel(own_ref, other_ref, mine_ref, feats_ref, scale_ref):
    half, model_width = own_ref.shape[0], feats_ref.shape[1]
    for part, rows_ref in enumerate((own_ref, other_ref)):
        here = pl.ds(part * half, half)
        feats_ref[here, :] = rows_ref[:, :model_width]
        tail = rows_ref[:, model_width:].astype(jnp.float32) * mine_ref[...]
        scale_ref[here, :] = jnp.sum(tail, axis=1, keepdims=True)


def join_rows(own_rows, other_rows, mine):
    half, width = own_rows.shape
    model_width = width - mine.shape[1]
    return pl.pallas_call(
        join_kernel,
        out_shape=(
            jax.ShapeDtypeStruct((2 * half, model_width), jnp.bfloat16),
            jax.ShapeDtypeStruct((2 * half, 1), jnp.float32),
        ),
        compiler_params=pltpu.CompilerParams(vmem_limit_bytes=24 * 1024 * 1024),
        cost_estimate=pl.CostEstimate(
            flops=2 * half * width, bytes_accessed=8 * half * width, transcendentals=0
        ),
    )(own_rows, other_rows, mine)


def body(tokens, node_ids, local_ids, affinity, w_gate, w_up, w_down, grad_parts):
    edp_count = lax.axis_size("edp")
    ep_count = lax.axis_size("ep")
    experts = edp_count * ep_count
    tok_rows, model_width = tokens.shape
    top_routes = local_ids.shape[1]
    node_pick = node_ids.shape[1]
    capacity = 10 * tok_rows // experts
    per_node = experts // GROUPS
    line = ep_count // per_node
    pairs = per_node // 2
    plane = edp_count * pairs
    f32, bf16 = jnp.float32, jnp.bfloat16

    edp_me, ep_me = lax.axis_index("edp"), lax.axis_index("ep")
    node_me = ep_me // per_node
    pair_me = (ep_me % per_node) // 2
    core_me = ep_me % 2
    me = edp_me * ep_count + ep_me
    plane_me = edp_me * pairs + pair_me

    def split(device):
        edp, ep = divmod(device, ep_count)
        node, inner = divmod(ep, per_node)
        pair, core = divmod(inner, 2)
        return edp, node, pair, core

    def join(edp, node, pair, core):
        return edp * ep_count + node * per_node + pair * 2 + core

    def along_line(value, step):
        perm = []
        for device in range(experts):
            edp, node, pair, core = split(device)
            perm.append((device, join(edp, node ^ step, pair, core)))
        return lax.ppermute(value, AXES, perm)

    def in_plane(value, step):
        perm = []
        for device in range(experts):
            edp, node, pair, core = split(device)
            other_edp, other_pair = divmod((edp * pairs + pair) ^ step, pairs)
            perm.append((device, join(other_edp, node, other_pair, core)))
        return lax.ppermute(value, AXES, perm)

    def core_swap(value):
        return lax.ppermute(value, AXES, [(device, device ^ 1) for device in range(experts)])

    def pick_row(value, index):
        return lax.dynamic_index_in_dim(value, index, 0, keepdims=False)

    grad_rows, grad_cols = grad_parts.shape[1:]
    grad_rows, grad_cols = grad_parts.shape[1:]
    grad = grad_parts[0].reshape(edp_count, line, pairs, 2, grad_rows * grad_cols // experts)
    grad = grad.transpose(3, 0, 2, 1, 4).reshape(2, plane, line, -1)
    grad = pick_row(grad, core_me) + core_swap(pick_row(grad, core_me ^ 1))
    total = pick_row(grad, plane_me)
    for step in range(1, plane):
        total = total + in_plane(pick_row(grad, plane_me ^ step), step)
    grad = total
    total = pick_row(grad, node_me)
    for step in range(1, line):
        total = total + along_line(pick_row(grad, node_me ^ step), step)
    router_grad = total.reshape(grad_rows // experts, grad_cols)

    expert = jnp.repeat(node_ids, top_routes // node_pick, axis=1) * per_node + local_ids
    weight = 2.5 * affinity / jnp.sum(affinity, axis=1, keepdims=True)
    every = jnp.arange(experts, dtype=jnp.int32)
    dense = jnp.sum(
        jnp.where(expert[:, :, None] == every[None, None, :], weight[:, :, None], 0.0), axis=1
    )
    high = lax.reduce_precision(dense, 8, 7)
    low = dense - high
    spare = -(2 * experts) % 128
    extended = jnp.concatenate(
        [tokens, high.astype(bf16), low.astype(bf16), jnp.zeros((tok_rows, spare), bf16)], axis=1
    )

    rows_iota = jnp.arange(tok_rows, dtype=jnp.int32)
    earlier = (rows_iota[:, None] < rows_iota[None, :]).astype(f32)
    plane_ids = plane_me ^ jnp.arange(plane, dtype=jnp.int32)
    first_expert = (
        (plane_ids // pairs) * ep_count + node_me * per_node + (plane_ids % pairs) * 2
    )
    pick = (first_expert[:, None] == every[None, :]).astype(f32)
    sent_iota = jnp.arange(plane * capacity, dtype=jnp.int32)
    spread = (sent_iota[:, None] // capacity == jnp.arange(plane)[None, :]).astype(f32)
    slot_of = jnp.broadcast_to(
        (sent_iota % capacity).astype(f32)[:, None], (plane * capacity, tok_rows)
    )
    tail_ids = jnp.arange(2 * experts + spare, dtype=jnp.int32)
    mine = ((tail_ids == me) | (tail_ids == me + experts)).astype(f32)[None, :]

    def dispatch(block):
        select, picked = select_rows(block, pick, earlier, spread, slot_of)
        picked = picked.reshape(plane, capacity, -1)
        got = [picked[0]] + [in_plane(picked[step], step) for step in range(1, plane)]
        own_rows = jnp.concatenate(got, axis=0)
        return select, own_rows, core_swap(own_rows)

    def expert_rows(own_rows, other_rows):
        half = own_rows.shape[0]
        feats, scale = join_rows(own_rows, other_rows, mine)
        gate_act = jnp.dot(feats, w_gate[0], preferred_element_type=f32)
        up_act = jnp.dot(feats, w_up[0], preferred_element_type=f32)
        hidden = (jax.nn.silu(gate_act) * up_act).astype(bf16)
        result = jnp.dot(hidden, w_down[0], preferred_element_type=f32)
        scaled = (result * scale).astype(bf16)
        other = core_swap(scaled[half:])
        return (scaled[:half].astype(f32) + other.astype(f32)).astype(bf16)

    def combine(select, summed):
        summed = summed.reshape(plane, capacity, model_width)
        back = [summed[0]] + [in_plane(summed[step], step) for step in range(1, plane)]
        back = jnp.concatenate(back, axis=0)
        return lax.dot_general(select, back, (((0,), (0,)), ((), ())), preferred_element_type=f32)

    blocks = [extended]
    for step in range(1, line):
        blocks.append(along_line(extended, step))
    mixed = jnp.zeros((tok_rows, model_width), f32)
    sent = [dispatch(block) for block in blocks]
    for chunk in range(line):
        select, own_rows, other_rows = sent[chunk]
        part = combine(select, expert_rows(own_rows, other_rows))
        if chunk:
            part = along_line(part.astype(bf16), chunk).astype(f32)
        mixed = mixed + part
    return (mixed.astype(bf16), router_grad)


def solution(mesh):
    placed = (
        P(("edp", "ep"), None),
        P(("edp", "ep"), None),
        P(("edp", "ep"), None),
        P(("edp", "ep"), None),
        P(("edp", "ep"), None, None),
        P(("edp", "ep"), None, None),
        P(("edp", "ep"), None, None),
        P(("edp", "ep"), None, None),
    )
    return jax.shard_map(
        body,
        mesh=mesh,
        in_specs=placed,
        out_specs=(P(("edp", "ep"), None), P(("edp", "ep"), None)),
        check_vma=False,
    )
```
